32 devices in a mesh: win: 32 (over z, y, x, core).
Axes of the slice: x: 2, y: 2, z: 4, core: 2. Of those that a mesh axis runs over, the one named last changes fastest.
Arguments:
- point_rows: int32 [64, 32768], P('win'), may hold values from 0 to 31
- point_cols: int32 [64, 32768], P('win'), may hold values from 0 to 1023
- point_chans: int32 [64, 32768], P('win'), may hold values from 0 to 3
- point_weights: bfloat16 [64, 32768], P('win'), may hold values from 0.25 to 4
- decay: float32 [64, 4], P('win'), may hold values from 0.3 to 1
Outputs:
- heat: float32 [64, 4, 32, 1024], P('win')
The draws below stay inside these ranges and needn't reach their ends.
All inputs are finite; a program needn't handle non-finite values.
Results may differ from the reference program's by a relative error of at most 0.0003.
Values sent between devices are 32-bit elements; how exact they have to be, the bound alone decides.
A program may use at most 64 MiB of HBM per device.

```python
import math
import jax
import jax.numpy as jnp
import numpy as np
from jax import lax

IMAGE_LAYERS = 4
COLS = 1024
ROWS = 32
P_DEV = 32768
PERIOD_COUNT = 64


def draw_decay(key, part):
    generator_seeds = jax.random.split(jax.random.fold_in(key, 77), 6)
    order = jax.random.permutation(generator_seeds[0], IMAGE_LAYERS)
    slow = order < IMAGE_LAYERS // 2
    slow_rate = jax.random.uniform(generator_seeds[1], (IMAGE_LAYERS,), jnp.float32, 0.2, 1.0) / PERIOD_COUNT
    fast_rate = 1.0 / jax.random.uniform(generator_seeds[2], (IMAGE_LAYERS,), jnp.float32, 8.0, 20.0)
    base = jnp.where(slow, slow_rate, fast_rate)
    jitter = jax.random.uniform(generator_seeds[3], (PERIOD_COUNT, IMAGE_LAYERS), jnp.float32, 0.5, 2.0)
    sudden_surge = jax.random.uniform(generator_seeds[4], (PERIOD_COUNT, IMAGE_LAYERS), jnp.float32) < 3.0 / PERIOD_COUNT
    fading_multiplier = jnp.where(sudden_surge, jax.random.uniform(generator_seeds[5], (PERIOD_COUNT, IMAGE_LAYERS), jnp.float32, 0.5, 0.8), 1.0)
    return (jnp.exp(-base[None, :] * jitter) * fading_multiplier).astype(jnp.float32)


def touch_ends(result, key, low, top_value):
    spot = [jax.random.randint(jax.random.fold_in(key, axis), (), 0, length) for axis, length in enumerate(result.shape)]
    main_axis = result.shape.index(max(result.shape))
    beside = spot[:main_axis] + [(spot[main_axis] + 1) % result.shape[main_axis]] + spot[main_axis + 1:]
    return result.at[tuple(spot)].set(low).at[tuple(beside)].set(top_value)


def block_levels(own_key, shape, pieces, low, high):
    def one(position, parts):
        draws = jax.random.uniform(jax.random.fold_in(jax.random.fold_in(own_key, 6), position), (parts,), jnp.float32, low / len(pieces), high / len(pieces))
        return jnp.repeat(jnp.exp(draws), shape[position] // parts).reshape((-1,) + (1,) * (len(shape) - position - 1))

    gain = one(*pieces[0])
    for cut in pieces[1:]:
        gain = gain * one(*cut)
    return gain


def cumulative_ranks(amount, slope):
    loads = [(1 << 20) // math.isqrt(grade ** slope) + 1 for grade in range(1, amount + 1)]
    width = 1 + sum(loads) // (1 << 30)
    return np.cumsum(np.array([max(1, weight // width) for weight in loads]))


def ranked(key, extent, number_of, skew):
    listing = cumulative_ranks(number_of, skew)
    pick = jax.random.randint(jax.random.fold_in(key, 1), extent, 0, int(listing[number_of - 1]))
    standing = jnp.searchsorted(jnp.asarray(listing, jnp.int32), pick, side="right")
    return jax.random.permutation(jax.random.fold_in(key, 2), number_of)[standing].astype(jnp.int32)


def setup_inputs(seed: int = 0) -> dict:
    arg_keys = jax.random.split(jax.random.key(seed), 6)
    point_rows = touch_ends(jax.random.randint(arg_keys[0], (PERIOD_COUNT, P_DEV), 0, ROWS), jax.random.fold_in(arg_keys[0], 1), 0, ROWS - 1).astype(jnp.int32)
    point_cols = touch_ends(ranked(arg_keys[1], (PERIOD_COUNT, P_DEV), COLS, 1), jax.random.fold_in(arg_keys[1], 3), 0, COLS - 1).astype(jnp.int32)
    point_chans = touch_ends(jax.random.randint(arg_keys[2], (PERIOD_COUNT, P_DEV), 0, IMAGE_LAYERS), jax.random.fold_in(arg_keys[2], 1), 0, IMAGE_LAYERS - 1).astype(jnp.int32)
    point_weights = jnp.clip(jnp.exp(math.log(4.0) - 2.7725887 * jax.random.uniform(arg_keys[3], (PERIOD_COUNT, P_DEV), jnp.float32) ** block_levels(arg_keys[3], (PERIOD_COUNT, P_DEV), ((0, 32),), -0.2, 0.2)), 0.25, 4.0).astype(jnp.bfloat16)
    decay = draw_decay(jax.random.fold_in(arg_keys[5], 71), 0)
    return {"point_rows": point_rows, "point_cols": point_cols, "point_chans": point_chans, "point_weights": point_weights, "decay": decay}


def reference(point_rows, point_cols, point_chans, point_weights, decay):
    flattened_index = (point_chans * ROWS + point_rows) * COLS + point_cols
    windows = point_rows.shape[0]
    window_ids = jnp.arange(windows, dtype=jnp.int32)[:, None] + jnp.zeros_like(flattened_index)
    hist = jnp.zeros((windows, IMAGE_LAYERS * ROWS * COLS), jnp.float32)
    hist = hist.at[window_ids, flattened_index].add(point_weights.astype(jnp.float32))
    hist = hist.reshape(windows, IMAGE_LAYERS, ROWS, COLS)

    def advance(carry, input_arrays):
        fading_multiplier, canvas = input_arrays
        carry = fading_multiplier[:, None, None] * carry + canvas
        return carry, carry

    start = jnp.zeros((IMAGE_LAYERS, ROWS, COLS), jnp.float32)
    final, heat = lax.scan(advance, start, (decay, hist))
    return heat
```

```python
import functools

import jax
import jax.numpy as jnp
from jax import lax
from jax.experimental import pallas as pl
from jax.experimental.pallas import tpu as pltpu
from jax.sharding import PartitionSpec as P

IMAGE_LAYERS = 4
COLS = 1024
ROWS = 32


def one_hot(index, size, on, points):
    spread = jnp.broadcast_to(index.astype(jnp.float32), (16, points)).astype(jnp.bfloat16)
    slots = lax.broadcasted_iota(jnp.int32, (16, points), 0).astype(jnp.float32).astype(jnp.bfloat16)
    off = jnp.zeros((16, points), jnp.bfloat16)
    return jnp.concatenate(
        [jnp.where(spread == slots + jnp.bfloat16(16.0 * g), on, off) for g in range(size // 16)], axis=0
    )


def bin_kernel(points, rows_ref, cols_ref, chans_ref, weights_ref, hist_ref):
    windows, total = rows_ref.shape
    slots = IMAGE_LAYERS * ROWS
    for window in range(windows):
        hist_ref[window] = jnp.zeros((slots, COLS), jnp.float32)

        def step(i, carry):
            here = pl.ds(pl.multiple_of(i * points, points), points)
            take = lambda ref: ref[window : window + 1, here]
            cols = take(cols_ref)
            cell = take(chans_ref) * ROWS + take(rows_ref) + (cols // 256) * slots
            weights = jnp.broadcast_to(take(weights_ref).astype(jnp.float32), (16, points)).astype(jnp.bfloat16)
            right = one_hot(cols % 256, 256, weights, points)
            for first in range(0, slots * COLS // 256, 256):
                left = one_hot(cell - first, 256, jnp.ones((16, points), jnp.bfloat16), points)
                part = lax.dot_general(
                    left, right, (((1,), (1,)), ((), ())), preferred_element_type=jnp.float32
                )
                for j in range(256 // slots):
                    at = (first // slots + j) * 256
                    hist_ref[window, :, at : at + 256] += part[j * slots : (j + 1) * slots]
            return carry

        lax.fori_loop(0, total // points, step, 0)


def bin_points(point_rows, point_cols, point_chans, point_weights):
    windows, total = point_rows.shape
    hist = pl.pallas_call(
        functools.partial(bin_kernel, min(4096, total)),
        out_shape=jax.ShapeDtypeStruct((windows, IMAGE_LAYERS * ROWS, COLS), jnp.float32),
        in_specs=[pl.BlockSpec(memory_space=pltpu.VMEM)] * 4,
        out_specs=pl.BlockSpec(memory_space=pltpu.VMEM),
        compiler_params=pltpu.CompilerParams(vmem_limit_bytes=48 * 2**20),
    )(point_rows, point_cols, point_chans, point_weights)
    return hist.reshape(windows, IMAGE_LAYERS, ROWS, COLS)


def affine_cells(earlier, later):
    return (earlier[0] * later[0], later[0] * earlier[1] + later[1])


def spread_factors(factors, first_cell, piece):
    channel_of = (first_cell + jnp.arange(piece, dtype=jnp.int32)) // (ROWS * COLS)
    spread = jnp.zeros((factors.shape[0], piece), jnp.float32)
    for channel in range(IMAGE_LAYERS):
        spread = spread + jnp.where(
            channel_of[None, :] == channel, factors[:, channel][:, None], 0.0
        )
    return spread


def finish(running, decay, hist):
    outputs = []
    for window in range(hist.shape[0]):
        running = decay[window][:, None, None] * running + hist[window]
        outputs.append(running)
    return jnp.stack(outputs, 0)


def summarize(decay, hist):
    shard_multiplier = jnp.ones((IMAGE_LAYERS,), jnp.float32)
    local_canvas = jnp.zeros((IMAGE_LAYERS, ROWS, COLS), jnp.float32)
    for window in range(hist.shape[0]):
        local_canvas = decay[window][:, None, None] * local_canvas + hist[window]
        shard_multiplier = shard_multiplier * decay[window]
    return (shard_multiplier, local_canvas)


def local(point_rows, point_cols, point_chans, point_weights, decay):
    cells = IMAGE_LAYERS * ROWS * COLS
    hist = bin_points(point_rows, point_cols, point_chans, point_weights)
    shard_multiplier, local_canvas = summarize(decay, hist)
    all_factors = lax.all_gather(shard_multiplier[None, :], "win", axis=0, tiled=True)
    owned = lax.all_to_all(
        local_canvas.reshape(1, cells), "win", split_axis=1, concat_axis=0, tiled=True
    )
    piece = owned.shape[1]
    cell_decay = spread_factors(all_factors, lax.axis_index("win") * piece, piece)
    inclusive = lax.associative_scan(affine_cells, (cell_decay, owned), axis=0)
    exclusive = jnp.concatenate([jnp.zeros((1, piece), jnp.float32), inclusive[1][:-1]], 0)
    returned = lax.all_to_all(exclusive, "win", split_axis=0, concat_axis=1, tiled=True)
    return finish(returned.reshape(IMAGE_LAYERS, ROWS, COLS), decay, hist)


def solution(mesh):
    placed = (P("win", None), P("win", None), P("win", None), P("win", None), P("win", None))
    return jax.shard_map(
        local, mesh=mesh, in_specs=placed, out_specs=P("win", None, None, None), check_vma=False
    )
```

```python
import functools

import jax
import jax.numpy as jnp
from jax import lax
from jax.experimental import pallas as pl
from jax.experimental.pallas import tpu as pltpu
from jax.sharding import PartitionSpec as P

IMAGE_LAYERS = 4
COLS = 1024
ROWS = 32
SLOTS = IMAGE_LAYERS * ROWS
LANES = 128
SUBLANES = 8
PART = 256
CHUNK = 512
POINTS = 8192
MESH = pl.DeviceIdType.MESH


def one_hot(index, size, on, points):
    spread = jnp.broadcast_to(index.astype(jnp.float32), (16, points)).astype(jnp.bfloat16)
    slots = lax.broadcasted_iota(jnp.int32, (16, points), 0).astype(jnp.float32).astype(jnp.bfloat16)
    off = jnp.zeros((16, points), jnp.bfloat16)
    return jnp.concatenate(
        [jnp.where(spread == slots + jnp.bfloat16(16.0 * g), on, off) for g in range(size // 16)], axis=0
    )


def bin_step(rows_ref, cols_ref, chans_ref, weights_ref, hist, window, chunk, first, points):
    here = pl.ds(pl.multiple_of(first, points), points)
    take = lambda ref: ref[window : window + 1, here]
    cols = take(cols_ref)
    cell = take(chans_ref) * ROWS + take(rows_ref) + (cols // PART - chunk * (CHUNK // PART)) * SLOTS
    cell = jnp.clip(cell, -1, CHUNK // PART * SLOTS)
    weights = jnp.broadcast_to(take(weights_ref).astype(jnp.float32), (16, points)).astype(jnp.bfloat16)
    right = one_hot(cols % PART, PART, weights, points)
    left = one_hot(cell, CHUNK // PART * SLOTS, jnp.ones((16, points), jnp.bfloat16), points)
    part = lax.dot_general(left, right, (((1,), (1,)), ((), ())), preferred_element_type=jnp.float32)
    for j in range(CHUNK // PART):
        hist[window, chunk, :, j * PART : (j + 1) * PART] += part[j * SLOTS : (j + 1) * SLOTS]


def across(tile, width):
    return jnp.concatenate([tile] * (width // LANES), axis=1)


def kernel(
    n, size, points,
    rows_hbm, cols_hbm, chans_hbm, weights_hbm, decay_ref, out_hbm,
    rows_ref, cols_ref, chans_ref, weights_ref, hist, stage, inbox, total, earlier, carried, spread, back, prefix,
    load_sem, store_sem, go_send, go_recv, up_send, up_recv, back_send, back_recv,
):
    windows, count = rows_ref.shape
    groups = n // size
    piece = SLOTS // size
    chunks = COLS // CHUNK
    me = lax.axis_index("win")
    group, member = lax.div(me, size), lax.rem(me, size)
    mate = lambda k: group * size + lax.rem(member + k, size)

    loads = [
        pltpu.make_async_copy(source, target, load_sem.at[i])
        for i, (source, target) in enumerate(
            ((cols_hbm, cols_ref), (chans_hbm, chans_ref), (rows_hbm, rows_ref), (weights_hbm, weights_ref))
        )
    ]
    for load in loads:
        load.start()

    barrier = pltpu.get_barrier_semaphore()
    for k in range(1, size):
        pl.semaphore_signal(barrier, inc=1, device_id=(mate(k),), device_id_type=MESH)
    for k in range(1, groups):
        pl.semaphore_signal(barrier, inc=1, device_id=(lax.rem(me + k * size, n),), device_id_type=MESH)

    hist[...] = jnp.zeros(hist.shape, jnp.float32)
    for load in loads:
        load.wait()
    pl.semaphore_wait(barrier, size - 1 + groups - 1)

    def go(chunk, k):
        peer = lax.rem(member + k, size)
        return pltpu.make_async_remote_copy(
            src_ref=stage.at[chunk, peer], dst_ref=inbox.at[chunk, member],
            send_sem=go_send.at[chunk, k], recv_sem=go_recv.at[chunk, member],
            device_id=(mate(k),), device_id_type=MESH,
        )

    def come(chunk, k):
        peer = lax.rem(member + k, size)
        return pltpu.make_async_remote_copy(
            src_ref=stage.at[chunk, peer], dst_ref=inbox.at[chunk, peer],
            send_sem=go_send.at[chunk, k], recv_sem=go_recv.at[chunk, peer],
            device_id=(mate(k),), device_id_type=MESH,
        )

    def up(chunk, k, slot):
        return pltpu.make_async_remote_copy(
            src_ref=total.at[chunk], dst_ref=earlier.at[chunk, slot],
            send_sem=up_send.at[chunk, k], recv_sem=up_recv.at[chunk, slot],
            device_id=(lax.rem(me + k * size, n),), device_id_type=MESH,
        )

    def give(chunk, k):
        peer = lax.rem(member + k, size)
        return pltpu.make_async_remote_copy(
            src_ref=back.at[chunk, peer], dst_ref=prefix.at[chunk, member],
            send_sem=back_send.at[chunk, k], recv_sem=back_recv.at[chunk, member],
            device_id=(mate(k),), device_id_type=MESH,
        )

    def get(chunk, k):
        peer = lax.rem(member + k, size)
        return pltpu.make_async_remote_copy(
            src_ref=back.at[chunk, peer], dst_ref=prefix.at[chunk, peer],
            send_sem=back_send.at[chunk, k], recv_sem=back_recv.at[chunk, peer],
            device_id=(mate(k),), device_id_type=MESH,
        )

    def send_sums(chunk):
        for p in range(size):
            channel = p * piece // ROWS
            at = slice(p * piece, (p + 1) * piece)
            running = hist[0, chunk, at, :]
            factor = jnp.full((piece, LANES), decay_ref[0, channel], jnp.float32)
            for window in range(1, windows):
                running = decay_ref[window, channel] * running + hist[window, chunk, at, :]
                factor = factor * decay_ref[window, channel]
            stage[chunk, p, :, :CHUNK] = running
            stage[chunk, p, :, CHUNK:] = factor
        for k in range(1, size):
            go(chunk, k).start()
        inbox[chunk, member] = stage[chunk, member]

    def scan_group(chunk):
        for k in range(1, size):
            come(chunk, k).wait_recv()
        running = jnp.zeros((piece, CHUNK), jnp.float32)
        factor = jnp.ones((piece, LANES), jnp.float32)
        for m in range(size):
            back[chunk, m] = running
            spread[chunk, m] = factor
            by = inbox[chunk, m, :, CHUNK:]
            running = across(by, CHUNK) * running + inbox[chunk, m, :, :CHUNK]
            factor = factor * by
        total[chunk, :, :CHUNK] = running
        total[chunk, :, CHUNK:] = factor
        for k in range(1, groups):

            @pl.when(group + k < groups)
            def _():
                up(chunk, k, group).start()

    def send_back(chunk):
        if groups > 1:
            carried[...] = jnp.zeros((piece, CHUNK), jnp.float32)
            for g in range(groups - 1):

                @pl.when(g < group)
                def _():
                    up(chunk, 1, g).wait_recv()
                    by = earlier[chunk, g, :, CHUNK:]
                    carried[...] = across(by, CHUNK) * carried[...] + earlier[chunk, g, :, :CHUNK]

            @pl.when(group > 0)
            def _():
                before = carried[...]
                for m in range(size):
                    back[chunk, m] += across(spread[chunk, m], CHUNK) * before

        for k in range(1, size):
            give(chunk, k).start()
        prefix[chunk, member] = back[chunk, member]

    def store(chunk, window):
        return pltpu.make_async_copy(
            hist.at[window, chunk],
            out_hbm.at[window, :, pl.ds(chunk * CHUNK, CHUNK)],
            store_sem.at[chunk, window],
        )

    def finish(chunk):
        for k in range(1, size):
            get(chunk, k).wait_recv()
        for p in range(size):
            channel = p * piece // ROWS
            at = slice(p * piece, (p + 1) * piece)
            running = prefix[chunk, p]
            for window in range(windows):
                running = decay_ref[window, channel] * running + hist[window, chunk, at, :]
                hist[window, chunk, at, :] = running
        for window in range(windows):
            store(chunk, window).start()

    steps = count // points
    for chunk in range(chunks):
        for window in range(windows):

            def step(i, carry):
                if chunk > 0 and window == windows - 1:

                    @pl.when(i == steps // 4)
                    def _():
                        scan_group(chunk - 1)

                    @pl.when(i == steps - 1)
                    def _():
                        send_back(chunk - 1)

                bin_step(
                    rows_ref, cols_ref, chans_ref, weights_ref, hist, window, chunk, i * points, points
                )
                return carry

            lax.fori_loop(0, steps, step, 0)
        send_sums(chunk)
        if chunk > 0:
            finish(chunk - 1)
    scan_group(chunks - 1)
    send_back(chunks - 1)
    finish(chunks - 1)

    for chunk in range(chunks):
        for window in range(windows):
            store(chunk, window).wait()
        for k in range(1, size):
            go(chunk, k).wait_send()
            give(chunk, k).wait_send()
        for k in range(1, groups):

            @pl.when(group + k < groups)
            def _():
                up(chunk, k, group).wait_send()


def local(n, point_rows, point_cols, point_chans, point_weights, decay):
    windows, count = point_rows.shape
    size = max(s for s in range(1, SLOTS // SUBLANES + 1) if n % s == 0 and SLOTS % (s * SUBLANES) == 0)
    groups = n // size
    piece, chunks = SLOTS // size, COLS // CHUNK
    wide = CHUNK + LANES
    dma = pltpu.SemaphoreType.DMA
    heat = pl.pallas_call(
        functools.partial(kernel, n, size, min(POINTS, count)),
        out_shape=jax.ShapeDtypeStruct((windows, SLOTS, COLS), jnp.float32),
        in_specs=[pl.BlockSpec(memory_space=pl.ANY)] * 4 + [pl.BlockSpec(memory_space=pltpu.SMEM)],
        out_specs=pl.BlockSpec(memory_space=pl.ANY),
        scratch_shapes=[
            pltpu.VMEM((windows, count), jnp.int32),
            pltpu.VMEM((windows, count), jnp.int32),
            pltpu.VMEM((windows, count), jnp.int32),
            pltpu.VMEM((windows, count), jnp.bfloat16),
            pltpu.VMEM((windows, chunks, SLOTS, CHUNK), jnp.float32),
            pltpu.VMEM((chunks, size, piece, wide), jnp.float32),
            pltpu.VMEM((chunks, size, piece, wide), jnp.float32),
            pltpu.VMEM((chunks, piece, wide), jnp.float32),
            pltpu.VMEM((chunks, groups, piece, wide), jnp.float32),
            pltpu.VMEM((piece, CHUNK), jnp.float32),
            pltpu.VMEM((chunks, size, piece, LANES), jnp.float32),
            pltpu.VMEM((chunks, size, piece, CHUNK), jnp.float32),
            pltpu.VMEM((chunks, size, piece, CHUNK), jnp.float32),
            dma((4,)),
            dma((chunks, windows)),
            dma((chunks, size)),
            dma((chunks, size)),
            dma((chunks, groups)),
            dma((chunks, groups)),
            dma((chunks, size)),
            dma((chunks, size)),
        ],
        compiler_params=pltpu.CompilerParams(
            collective_id=0, has_side_effects=True, vmem_limit_bytes=56 * 2**20
        ),
    )(point_rows, point_cols, point_chans, point_weights, decay)
    return heat.reshape(windows, IMAGE_LAYERS, ROWS, COLS)


def solution(mesh):
    placed = (P("win", None), P("win", None), P("win", None), P("win", None), P("win", None))
    return jax.shard_map(
        functools.partial(local, mesh.shape["win"]),
        mesh=mesh, in_specs=placed, out_specs=P("win", None, None, None), check_vma=False,
    )
```

```python
import functools

import jax
import jax.numpy as jnp
from jax import lax
from jax.experimental import pallas as pl
from jax.experimental.pallas import tpu as pltpu
from jax.sharding import PartitionSpec as P

IMAGE_LAYERS = 4
COLS = 1024
ROWS = 32
SLOTS = IMAGE_LAYERS * ROWS
LANES = 128
SUBLANES = 8
PART = 256
CHUNK = 512
POINTS = 16384
MESH = pl.DeviceIdType.MESH


def one_hot(index, size, on, points):
    spread = jnp.broadcast_to(index.astype(jnp.float32), (16, points)).astype(jnp.bfloat16)
    slots = lax.broadcasted_iota(jnp.int32, (16, points), 0).astype(jnp.float32).astype(jnp.bfloat16)
    off = jnp.zeros((16, points), jnp.bfloat16)
    return jnp.concatenate(
        [jnp.where(spread == slots + jnp.bfloat16(16.0 * g), on, off) for g in range(size // 16)], axis=0
    )


def bin_step(rows_ref, cols_ref, chans_ref, weights_ref, hist, window, chunk, first, points):
    here = pl.ds(pl.multiple_of(first, points), points)
    take = lambda ref: ref[window : window + 1, here]
    cols = take(cols_ref)
    cell = take(chans_ref) * ROWS + take(rows_ref) + (cols // PART - chunk * (CHUNK // PART)) * SLOTS
    cell = jnp.clip(cell, -1, CHUNK // PART * SLOTS)
    weights = jnp.broadcast_to(take(weights_ref).astype(jnp.float32), (16, points)).astype(jnp.bfloat16)
    right = one_hot(cols % PART, PART, weights, points)
    left = one_hot(cell, CHUNK // PART * SLOTS, jnp.ones((16, points), jnp.bfloat16), points)
    part = lax.dot_general(left, right, (((1,), (1,)), ((), ())), preferred_element_type=jnp.float32)
    for j in range(CHUNK // PART):
        hist[window, chunk, :, j * PART : (j + 1) * PART] += part[j * SLOTS : (j + 1) * SLOTS]


def across(tile, width):
    return jnp.concatenate([tile] * (width // LANES), axis=1)


def kernel(
    n, size, points,
    rows_hbm, cols_hbm, chans_hbm, weights_hbm, decay_ref, out_hbm,
    rows_ref, cols_ref, chans_ref, weights_ref, hist, stage, inbox, total, earlier, carried, spread, back, prefix,
    load_sem, store_sem, go_send, go_recv, up_send, up_recv, back_send, back_recv,
):
    windows, count = rows_ref.shape
    groups = n // size
    piece = SLOTS // size
    chunks = COLS // CHUNK
    me = lax.axis_index("win")
    group, member = lax.div(me, size), lax.rem(me, size)
    mate = lambda k: group * size + lax.rem(member + k, size)

    sources = ((cols_hbm, cols_ref), (chans_hbm, chans_ref), (rows_hbm, rows_ref), (weights_hbm, weights_ref))
    loads = [
        pltpu.make_async_copy(source, target, load_sem.at[i]) for i, (source, target) in enumerate(sources)
    ]
    for load in loads:
        load.start()

    barrier = pltpu.get_barrier_semaphore()
    for k in range(1, size):
        pl.semaphore_signal(barrier, inc=1, device_id=(mate(k),), device_id_type=MESH)
    for k in range(1, groups):
        pl.semaphore_signal(barrier, inc=1, device_id=(lax.rem(me + k * size, n),), device_id_type=MESH)

    hist[...] = jnp.zeros(hist.shape, jnp.float32)
    for load in loads:
        load.wait()

    def sent(ref, chunk):
        return ref if chunk == 0 else ref.at[:, pl.ds(0, CHUNK)]

    def go(chunk, k):
        peer = lax.rem(member + k, size)
        return pltpu.make_async_remote_copy(
            src_ref=sent(stage.at[chunk, peer], chunk), dst_ref=sent(inbox.at[chunk, member], chunk),
            send_sem=go_send.at[chunk, k], recv_sem=go_recv.at[chunk, member],
            device_id=(mate(k),), device_id_type=MESH,
        )

    def come(chunk, k):
        peer = lax.rem(member + k, size)
        return pltpu.make_async_remote_copy(
            src_ref=sent(stage.at[chunk, peer], chunk), dst_ref=sent(inbox.at[chunk, peer], chunk),
            send_sem=go_send.at[chunk, k], recv_sem=go_recv.at[chunk, peer],
            device_id=(mate(k),), device_id_type=MESH,
        )

    def up(chunk, k, slot):
        return pltpu.make_async_remote_copy(
            src_ref=sent(total.at[chunk], chunk), dst_ref=sent(earlier.at[chunk, slot], chunk),
            send_sem=up_send.at[chunk, k], recv_sem=up_recv.at[chunk, slot],
            device_id=(lax.rem(me + k * size, n),), device_id_type=MESH,
        )

    def give(chunk, k):
        peer = lax.rem(member + k, size)
        return pltpu.make_async_remote_copy(
            src_ref=back.at[chunk, peer], dst_ref=prefix.at[chunk, member],
            send_sem=back_send.at[chunk, k], recv_sem=back_recv.at[chunk, member],
            device_id=(mate(k),), device_id_type=MESH,
        )

    def get(chunk, k):
        peer = lax.rem(member + k, size)
        return pltpu.make_async_remote_copy(
            src_ref=back.at[chunk, peer], dst_ref=prefix.at[chunk, peer],
            send_sem=back_send.at[chunk, k], recv_sem=back_recv.at[chunk, peer],
            device_id=(mate(k),), device_id_type=MESH,
        )

    def send_sums(chunk):
        for p in range(size):
            channel = p * piece // ROWS
            at = slice(p * piece, (p + 1) * piece)
            running = hist[0, chunk, at, :]
            factor = jnp.full((piece, LANES), decay_ref[0, channel], jnp.float32)
            for window in range(1, windows):
                running = decay_ref[window, channel] * running + hist[window, chunk, at, :]
                factor = factor * decay_ref[window, channel]
            stage[chunk, p, :, :CHUNK] = running
            if chunk == 0:
                stage[chunk, p, :, CHUNK:] = factor
        if chunk == 0:
            pl.semaphore_wait(barrier, size - 1 + groups - 1)
        for k in range(1, size):
            go(chunk, k).start()
        wide = CHUNK if chunk else CHUNK + LANES
        inbox[chunk, member, :, :wide] = stage[chunk, member, :, :wide]

    def scan_group(chunk):
        for k in range(1, size):
            come(chunk, k).wait_recv()
        running = jnp.zeros((piece, CHUNK), jnp.float32)
        factor = jnp.ones((piece, LANES), jnp.float32)
        for m in range(size):
            back[chunk, m] = running
            by = inbox[0, m, :, CHUNK:]
            if chunk == 0:
                spread[m] = factor
            running = across(by, CHUNK) * running + inbox[chunk, m, :, :CHUNK]
            if chunk == 0:
                factor = factor * by
        total[chunk, :, :CHUNK] = running
        if chunk == 0:
            total[chunk, :, CHUNK:] = factor
        for k in range(1, groups):

            @pl.when(group + k < groups)
            def _():
                up(chunk, k, group).start()

    def send_back(chunk):
        if groups > 1:
            carried[...] = jnp.zeros((piece, CHUNK), jnp.float32)
            for g in range(groups - 1):

                @pl.when(g < group)
                def _():
                    up(chunk, 1, g).wait_recv()
                    by = earlier[0, g, :, CHUNK:]
                    carried[...] = across(by, CHUNK) * carried[...] + earlier[chunk, g, :, :CHUNK]

            @pl.when(group > 0)
            def _():
                before = carried[...]
                for m in range(size):
                    back[chunk, m] += across(spread[m], CHUNK) * before

        for k in range(1, size):
            give(chunk, k).start()
        prefix[chunk, member] = back[chunk, member]

    def store(chunk, window):
        return pltpu.make_async_copy(
            hist.at[window, chunk],
            out_hbm.at[window, :, pl.ds(chunk * CHUNK, CHUNK)],
            store_sem.at[chunk, window],
        )

    def finish(chunk):
        for k in range(1, size):
            get(chunk, k).wait_recv()
        for p in range(size):
            channel = p * piece // ROWS
            at = slice(p * piece, (p + 1) * piece)
            running = prefix[chunk, p]
            for window in range(windows):
                running = decay_ref[window, channel] * running + hist[window, chunk, at, :]
                hist[window, chunk, at, :] = running
        for window in range(windows):
            store(chunk, window).start()

    steps = count // points
    for chunk in range(chunks):
        for window in range(windows):

            if chunk > 0 and window == windows - 1:
                scan_group(chunk - 1)

            def step(i, carry):
                if chunk > 0 and window == windows - 1 and steps > 1:

                    @pl.when(i == steps - 1)
                    def _():
                        send_back(chunk - 1)

                bin_step(
                    rows_ref, cols_ref, chans_ref, weights_ref, hist, window, chunk, i * points, points
                )
                return carry

            lax.fori_loop(0, steps, step, 0)
        send_sums(chunk)
        if chunk > 0:
            if steps == 1:
                send_back(chunk - 1)
            finish(chunk - 1)
    scan_group(chunks - 1)
    send_back(chunks - 1)
    finish(chunks - 1)

    for chunk in range(chunks):
        for window in range(windows):
            store(chunk, window).wait()
        for k in range(1, size):
            go(chunk, k).wait_send()
            give(chunk, k).wait_send()
        for k in range(1, groups):

            @pl.when(group + k < groups)
            def _():
                up(chunk, k, group).wait_send()


def local(n, point_rows, point_cols, point_chans, point_weights, decay):
    windows, count = point_rows.shape
    size = max(s for s in range(1, SLOTS // SUBLANES + 1) if n % s == 0 and SLOTS % (s * SUBLANES) == 0)
    groups = n // size
    piece, chunks = SLOTS // size, COLS // CHUNK
    wide = CHUNK + LANES
    dma = pltpu.SemaphoreType.DMA
    heat = pl.pallas_call(
        functools.partial(kernel, n, size, min(POINTS, count)),
        out_shape=jax.ShapeDtypeStruct((windows, SLOTS, COLS), jnp.float32),
        in_specs=[pl.BlockSpec(memory_space=pl.ANY)] * 4 + [pl.BlockSpec(memory_space=pltpu.SMEM)],
        out_specs=pl.BlockSpec(memory_space=pl.ANY),
        scratch_shapes=[
            pltpu.VMEM((windows, count), jnp.int32),
            pltpu.VMEM((windows, count), jnp.int32),
            pltpu.VMEM((windows, count), jnp.int32),
            pltpu.VMEM((windows, count), jnp.bfloat16),
            pltpu.VMEM((windows, chunks, SLOTS, CHUNK), jnp.float32),
            pltpu.VMEM((chunks, size, piece, wide), jnp.float32),
            pltpu.VMEM((chunks, size, piece, wide), jnp.float32),
            pltpu.VMEM((chunks, piece, wide), jnp.float32),
            pltpu.VMEM((chunks, groups, piece, wide), jnp.float32),
            pltpu.VMEM((piece, CHUNK), jnp.float32),
            pltpu.VMEM((size, piece, LANES), jnp.float32),
            pltpu.VMEM((chunks, size, piece, CHUNK), jnp.float32),
            pltpu.VMEM((chunks, size, piece, CHUNK), jnp.float32),
            dma((4,)),
            dma((chunks, windows)),
            dma((chunks, size)),
            dma((chunks, size)),
            dma((chunks, groups)),
            dma((chunks, groups)),
            dma((chunks, size)),
            dma((chunks, size)),
        ],
        compiler_params=pltpu.CompilerParams(
            collective_id=0, has_side_effects=True, vmem_limit_bytes=56 * 2**20
        ),
    )(point_rows, point_cols, point_chans, point_weights, decay)
    return heat.reshape(windows, IMAGE_LAYERS, ROWS, COLS)


def solution(mesh):
    placed = (P("win", None), P("win", None), P("win", None), P("win", None), P("win", None))
    return jax.shard_map(
        functools.partial(local, mesh.shape["win"]),
        mesh=mesh, in_specs=placed, out_specs=P("win", None, None, None), check_vma=False,
    )
```
